32 devices in a mesh: rep: 4 (over x, core), dp: 4 (over z), tp: 2 (over y).
Axes of the slice: x: 2, y: 2, z: 4, core: 2. Of those that a mesh axis runs over, the one named last changes fastest.
Arguments:
- hidden: bfloat16 [4, 512, 14336], P('rep', None, 'tp'), may hold values from -6 to 6
- down_weight: bfloat16 [14336, 8192], P('tp', 'dp'), may hold values from -0.046875 to 0.046875
- out_grad: bfloat16 [4, 512, 8192], P('rep', 'tp', 'dp'), may hold values from -6 to 6
- pseudo_grad: bfloat16 [4, 14336, 8192], P('rep', 'tp', 'dp'), may hold values from -6 to 6
- momentum: float32 [14336, 8192], P(('tp', 'rep'), 'dp'), may hold values from -6 to 6
Outputs:
- layer_out: bfloat16 [4, 512, 8192], P('rep', 'tp', 'dp')
- hidden_grad: bfloat16 [4, 512, 14336], P('rep', 'dp', 'tp')
- new_momentum: float32 [14336, 8192], P(('tp', 'rep'), 'dp')
- outer_step: bfloat16 [14336, 8192], P('tp', 'dp')
The draws below stay inside these ranges and needn't reach their ends.
All inputs are finite; a program needn't handle non-finite values.
Results may differ from the reference program's by a relative error of at most 0.017.
Values may be sent and summed in bfloat16 or wider, within the bound.
A program may use at most 256 MiB of HBM per device.

```python
import jax
import jax.numpy as jnp
from jax import lax

D = 8192
FF = 14336
TOKENS = 512
N_REP = 4
N_DP = 4
N_TP = 2


def block_scale(key, extent, cuts, low, largest):
    gain = 1.0
    for axis_at, parts in cuts:
        heights = jax.random.uniform(jax.random.fold_in(jax.random.fold_in(key, 6), axis_at), (parts,), jnp.float32, low / len(cuts), largest / len(cuts))
        gain = gain * jnp.repeat(jnp.exp(heights), extent[axis_at] // parts).reshape((-1,) + (1,) * (len(extent) - 1 - axis_at))
    return gain


def bell_draw(rng, dims, spread, reach, cuts=(), kind=jnp.bfloat16):
    level = block_scale(rng, dims, cuts, -0.22, 0.18) if cuts else 1.0
    array = jax.random.normal(rng, dims, jnp.float32) * spread * level
    return jnp.minimum(jnp.maximum(array, -reach), reach).astype(kind)


def setup_inputs(seed: int = 0) -> dict:
    key_list = jax.random.split(jax.random.key(seed), 6)
    return {
        "hidden": bell_draw(key_list[0], (N_REP, TOKENS, FF), 1.0, 6.0, ((0, 4), (2, 2))),
        "down_weight": bell_draw(key_list[1], (FF, D), FF ** -0.5, 0.046875, ((0, 2), (1, 4))),
        "out_grad": bell_draw(key_list[2], (N_REP, TOKENS, D), 1.0, 6.0, ((0, 4), (1, 2), (2, 4))),
        "pseudo_grad": bell_draw(key_list[3], (N_REP, FF, D), 1.0, 6.0, ((0, 4), (1, 2), (2, 4))),
        "momentum": bell_draw(key_list[4], (FF, D), 1.0, 6.0, ((0, 8), (1, 4)), jnp.float32),
    }


outer_rate = 0.7
momentum_rate = 0.9


def reference(hidden, down_weight, out_grad, pseudo_grad, momentum):
    hidden_width = FF // N_TP
    model_width = D // N_DP
    weight_tp = down_weight.reshape(N_TP, hidden_width, D)
    weight_dp = jnp.transpose(down_weight.reshape(FF, N_DP, model_width), (1, 0, 2))

    def forward_block(paired):
        return jnp.dot(paired[0], paired[1], preferred_element_type=jnp.float32).astype(jnp.bfloat16)

    def backward_block(paired):
        product = lax.dot_general(paired[0], paired[1], (((1,), (1,)), ((), ())), preferred_element_type=jnp.float32)
        return product.astype(jnp.bfloat16)

    def one_replica(paired):
        token_rows = paired[0]
        grad_rows = paired[1]
        rows_tp = jnp.transpose(token_rows.reshape(TOKENS, N_TP, hidden_width), (1, 0, 2))
        partial_out = lax.map(forward_block, (rows_tp, weight_tp))
        layer = jnp.sum(partial_out.astype(jnp.float32), axis=0).astype(jnp.bfloat16)
        grads_dp = jnp.transpose(grad_rows.reshape(TOKENS, N_DP, model_width), (1, 0, 2))
        partial_back = lax.map(backward_block, (grads_dp, weight_dp))
        back = jnp.sum(partial_back.astype(jnp.float32), axis=0).astype(jnp.bfloat16)
        return layer, back

    layer_out, hidden_grad = lax.map(one_replica, (hidden, out_grad))

    def accumulate(index, running_sum):
        return running_sum + pseudo_grad[index].astype(jnp.float32)

    totals = lax.fori_loop(0, N_REP, accumulate, jnp.zeros((FF, D), jnp.float32))
    average = totals / N_REP
    new_momentum = momentum_rate * momentum + average
    outer_step = (outer_rate * (average + momentum_rate * new_momentum)).astype(jnp.bfloat16)
    return layer_out, hidden_grad, new_momentum, outer_step
```

```python
import functools

import jax
import jax.numpy as jnp
from jax import lax
from jax.experimental import pallas as pl
from jax.experimental.pallas import tpu as pltpu
from jax.sharding import PartitionSpec as P

outer_rate = 0.7
momentum_rate = 0.9

copy_flops = 1000
n_groups = 4
whole_vmem = 2**26 - 2**16

MESH = pl.DeviceIdType.MESH
f32 = jnp.float32
bf16 = jnp.bfloat16


def pieces(extent, unit, most):
    return max(k for k in range(1, most + 1) if extent % (k * unit) == 0)


def kernel(
    n_rep, n_dp, n_tp, n_k, n_late, n_f, groups,
    hidden, weight, grads, pseudo, momentum,
    layer_out, hidden_grad, new_momentum, outer_step, xch, *refs,
):
    n_x, n_g = n_rep // 2, len(groups)
    late, edge, refs = refs[:n_g], refs[n_g:n_g + n_x - 1], refs[n_g + n_x - 1:]
    body(n_rep, n_dp, n_tp, n_k, n_late, n_f, groups,
         hidden, weight, grads, pseudo, momentum,
         layer_out, hidden_grad, new_momentum, outer_step, xch, late, edge, *refs)


def body(
    n_rep, n_dp, n_tp, n_k, n_late, n_f, groups,
    hidden, weight, grads, pseudo, momentum,
    layer_out, hidden_grad, new_momentum, outer_step, xch, late, edge,
    ps, pr, xv, la, lb, mom, nmb, wb, hb, gf, acc, po, tr, pb, dr,
    ld_sem, xs_sem, xr_sem, ps_sem, pr_sem, ss_sem, sr_sem, fs_sem, fr_sem, own_sem,
    gs_sem, gr_sem, ts_sem, tr_sem, ds_sem, dr_sem,
):
    n_x = n_rep // 2
    rep, dp, tp = lax.axis_index("rep"), lax.axis_index("dp"), lax.axis_index("tp")
    x, core = rep // 2, lax.rem(rep, 2)
    partner = 2 * x + 1 - core
    share, cols = momentum.shape
    chunk = share // n_k
    ffn = weight.shape[0]
    fb = ffn // n_f
    tokens = hidden.shape[1]
    t_rows, d_rows = tokens // n_tp, tokens // n_dp
    row_unit = 16
    n_sent = n_k - n_late
    sent = pl.ds(0, n_sent * chunk)

    def chip(d):
        return lax.rem(x + d, n_x)

    def rep_peer(d):
        return 2 * chip(d) + core

    def rows(owner, k):
        return pl.ds(pl.multiple_of(owner * share + k * chunk, chunk), chunk)

    def part(k):
        return pl.ds(pl.multiple_of(k * chunk, chunk), chunk)

    def remote(src, dst, send, recv, axis, index):
        return pltpu.make_async_remote_copy(
            src_ref=src, dst_ref=dst, send_sem=send, recv_sem=recv,
            device_id={axis: index}, device_id_type=MESH,
        )

    def drain(ref, sem):
        pltpu.make_async_copy(ref, ref, sem).wait()

    def own_rows(t, slot):
        d, k = 1 + lax.rem(t, n_x - 1), t // (n_x - 1)
        return pltpu.make_async_copy(
            pseudo.at[0, rows(rep_peer(d), k)], la.at[slot], ld_sem.at[slot]
        )

    own_rows(0, 0).start()
    barrier = pltpu.get_barrier_semaphore()
    peers = [("rep", partner)]
    peers += [("rep", rep_peer(d)) for d in range(1, n_x)]
    peers += [("dp", lax.rem(dp + d, n_dp)) for d in range(1, n_dp)]
    peers += [("tp", lax.rem(tp + d, n_tp)) for d in range(1, n_tp)]
    for axis, index in peers:
        pl.semaphore_signal(barrier, inc=1, device_id={axis: index}, device_id_type=MESH)
    pl.semaphore_wait(barrier, len(peers))

    def exchange(d, k):
        return remote(
            pseudo.at[0, rows(2 * chip(d) + 1 - core, k)], xv.at[d - 1, part(k)],
            xs_sem, xr_sem.at[d, k], "rep", partner,
        )

    def own_exchange(k):
        return remote(
            pseudo.at[0, rows(partner, k)], xch.at[part(k)],
            xs_sem, xr_sem.at[0, k], "rep", partner,
        )

    def start_exchange(k, carry):
        for d in range(1, n_x):
            exchange(d, k).start()
        return carry

    def start_own_exchange(k, carry):
        own_exchange(k).start()
        return carry

    lax.fori_loop(0, n_k, start_exchange, 0)

    mine = pl.ds(pl.multiple_of(tp * t_rows, t_rows), t_rows)

    def gather(d):
        return remote(grads.at[0], gf.at[mine], gs_sem.at[d - 1], gr_sem.at[d - 1],
                      "tp", lax.rem(tp + d, n_tp))

    for d in range(1, n_tp):
        gather(d).start()
    own_grads = pltpu.make_async_copy(grads.at[0], gf.at[mine], own_sem)
    own_grads.start()
    lax.fori_loop(0, n_k, start_own_exchange, 0)

    def partial_send(d, k):
        return remote(ps.at[d - 1, part(k)], pr.at[d - 1, part(k)], ps_sem,
                      pr_sem.at[d - 1, k], "rep", rep_peer(d))

    def reduce_chunk(t, carry):
        d, k = 1 + lax.rem(t, n_x - 1), t // (n_x - 1)
        slot = lax.rem(t, 2)

        @pl.when(t + 1 < n_k * (n_x - 1))
        def _():
            own_rows(t + 1, 1 - slot).start()

        own_rows(t, slot).wait()
        exchange(d, k).wait_recv()

        def add(i, c):
            r = pl.ds(pl.multiple_of(i * row_unit, row_unit), row_unit)
            o = pl.ds(pl.multiple_of(k * chunk + i * row_unit, row_unit), row_unit)
            total = la[slot, r, :].astype(f32) + xv[d - 1, o, :].astype(f32)
            ps[d - 1, o, :] = total.astype(bf16)
            return c

        lax.fori_loop(0, chunk // row_unit, add, 0)
        partial_send(d, k).start()
        return carry

    lax.fori_loop(0, n_k * (n_x - 1), reduce_chunk, 0)

    tn = cols // pieces(cols, 128, max(1, cols // 512))
    tm = tokens // pieces(tokens, row_unit, 2)

    def clear(i, carry):
        r = pl.ds(pl.multiple_of(i * row_unit, row_unit), row_unit)
        acc[r, :] = jnp.zeros((row_unit, cols), f32)
        return carry

    lax.fori_loop(0, tokens // row_unit, clear, 0)
    own_grads.wait()
    for d in range(1, n_tp):
        gather(d).wait()

    def back_send(d, f):
        to = lax.rem(dp + d, n_dp)
        c = pl.ds(pl.multiple_of(f * fb, fb), fb)
        return remote(
            pb.at[pl.ds(pl.multiple_of(to * d_rows, d_rows), d_rows), c],
            dr.at[d - 1, :, c], ds_sem, dr_sem.at[d - 1], "dp", to,
        )

    def matmul_block(f, carry):
        c = pl.ds(pl.multiple_of(f * fb, fb), fb)
        a = pltpu.make_async_copy(weight.at[c], wb, ld_sem.at[0])
        b = pltpu.make_async_copy(hidden.at[0, :, c], hb, ld_sem.at[1])
        a.start()
        b.start()
        a.wait()
        b.wait()

        def back(m, z):
            r = pl.ds(pl.multiple_of(m * tm, tm), tm)
            product = lax.dot_general(
                gf[r, :], wb[...], (((1,), (1,)), ((), ())), preferred_element_type=f32
            )
            pb[r, c] = product.astype(bf16)
            return z

        lax.fori_loop(0, tokens // tm, back, 0)
        for d in range(1, n_dp):
            back_send(d, f).start()

        def forward(n, z):
            t = pl.ds(pl.multiple_of(n * tn, tn), tn)
            acc[:, t] += jnp.dot(hb[...], wb[:, t], preferred_element_type=f32)
            return z

        lax.fori_loop(0, cols // tn, forward, 0)
        return carry

    lax.fori_loop(0, n_f, matmul_block, 0)

    def round_out(i, carry):
        r = pl.ds(pl.multiple_of(i * row_unit, row_unit), row_unit)
        po[r, :] = acc[r, :].astype(bf16)
        return carry

    lax.fori_loop(0, tokens // row_unit, round_out, 0)

    def out_send(d):
        to = lax.rem(tp + d, n_tp)
        return remote(po.at[pl.ds(pl.multiple_of(to * t_rows, t_rows), t_rows)],
                      tr.at[d - 1], ts_sem.at[d - 1], tr_sem.at[d - 1], "tp", to)

    for d in range(1, n_tp):
        out_send(d).start()

    def store_momentum(k):
        return pltpu.make_async_copy(nmb, new_momentum.at[part(k)], ld_sem.at[3])

    def step_send(d, k):
        return remote(pr.at[0, part(k)], outer_step.at[rows(rep, k)], ss_sem,
                      sr_sem.at[d - 1, k], "rep", rep_peer(d))

    def edge_send(d):
        return remote(pr.at[0, part(n_sent - 1)], edge[d - 1], ss_sem,
                      sr_sem.at[d - 1, n_sent - 1], "rep", rep_peer(d))

    def update_chunk(k, carry):
        a = pltpu.make_async_copy(pseudo.at[0, rows(rep, k)], la.at[0], ld_sem.at[0])
        m = pltpu.make_async_copy(momentum.at[part(k)], mom, ld_sem.at[2])
        a.start()
        m.start()
        own_exchange(k).wait_recv()
        b = pltpu.make_async_copy(xch.at[part(k)], lb, ld_sem.at[1])
        b.start()
        for d in range(1, n_x):
            partial_send(d, k).wait_recv()

        @pl.when(k > 0)
        def _():
            store_momentum(k - 1).wait()

        a.wait()
        b.wait()
        m.wait()

        def update(i, c):
            r = pl.ds(pl.multiple_of(i * row_unit, row_unit), row_unit)
            o = pl.ds(pl.multiple_of(k * chunk + i * row_unit, row_unit), row_unit)
            total = la[0, r, :].astype(f32) + lb[r, :].astype(f32)
            for d in range(1, n_x):
                total += pr[d - 1, o, :].astype(f32)
            average = total / n_rep
            fresh = momentum_rate * mom[r, :] + average
            nmb[r, :] = fresh
            pr[0, o, :] = (outer_rate * (average + momentum_rate * fresh)).astype(bf16)
            return c

        lax.fori_loop(0, chunk // row_unit, update, 0)

        @pl.when(k < n_sent - 1)
        def _():
            for d in range(1, n_x):
                step_send(d, k).start()

        @pl.when(k == n_sent - 1)
        def _():
            for d in range(1, n_x):
                edge_send(d).start()

        @pl.when(k < n_sent)
        def _():
            remote(pr.at[0, part(k)], outer_step.at[rows(rep, k)], fs_sem, fr_sem,
                   "rep", partner).start()
            pltpu.make_async_copy(
                pr.at[0, part(k)], outer_step.at[rows(rep, k)], own_sem
            ).start()

        store_momentum(k).start()
        return carry

    lax.fori_loop(0, n_k, update_chunk, 0)
    store_momentum(n_k - 1).wait()
    late_copies = [
        pltpu.make_async_copy(
            pr.at[0, pl.ds(n_sent * chunk + start, size)], target, ld_sem.at[4 + g]
        )
        for g, ((start, size), target) in enumerate(zip(groups, late))
    ]
    for copy in late_copies:
        copy.start()

    def forward_chunk(k, carry):
        for d in range(1, n_x):
            step_send(d, k).wait_recv()
            r = rows(2 * chip(n_x - d) + core, k)
            remote(outer_step.at[r], outer_step.at[r], fs_sem, fr_sem, "rep", partner).start()
        return carry

    lax.fori_loop(0, n_sent // 2, forward_chunk, 0)

    for d in range(1, n_tp):
        out_send(d).wait()

    def sum_out(i, carry):
        r = pl.ds(pl.multiple_of(i * row_unit, row_unit), row_unit)
        o = pl.ds(pl.multiple_of(tp * t_rows + i * row_unit, row_unit), row_unit)
        total = po[o, :].astype(f32)
        for d in range(1, n_tp):
            total += tr[d - 1, r, :].astype(f32)
        tr[0, r, :] = total.astype(bf16)
        return carry

    lax.fori_loop(0, t_rows // row_unit, sum_out, 0)
    out_copy = pltpu.make_async_copy(tr.at[0], layer_out.at[0], ld_sem.at[0])
    out_copy.start()

    for d in range(1, n_dp):
        drain(dr.at[d - 1], dr_sem.at[d - 1])

    def sum_back(f, carry):
        c = pl.ds(pl.multiple_of(f * fb, fb), fb)

        def band(i, z):
            r = pl.ds(pl.multiple_of(i * row_unit, row_unit), row_unit)
            o = pl.ds(pl.multiple_of(dp * d_rows + i * row_unit, row_unit), row_unit)
            total = pb[o, c].astype(f32)
            for d in range(1, n_dp):
                total += dr[d - 1, r, c].astype(f32)
            dr[0, r, c] = total.astype(bf16)
            return z

        lax.fori_loop(0, d_rows // row_unit, band, 0)
        return carry

    lax.fori_loop(0, n_f, sum_back, 0)
    back_copy = pltpu.make_async_copy(dr.at[0], hidden_grad.at[0], ld_sem.at[1])
    back_copy.start()

    lax.fori_loop(n_sent // 2, n_sent - 1, forward_chunk, 0)

    out_copy.wait()
    back_copy.wait()
    for copy in late_copies:
        copy.wait()
    drain(outer_step.at[pl.ds(0, n_x * share)], xs_sem)
    drain(ps, ps_sem)
    drain(ps.at[:, sent], ss_sem)
    forwarded = pl.ds(0, (n_x * n_sent - n_x + 1) * chunk)
    drain(outer_step.at[forwarded], fs_sem)
    drain(outer_step.at[forwarded], fr_sem)
    for d in range(1, n_x):
        edge_send(d).wait_recv()
    drain(pr.at[0, sent], own_sem)
    drain(dr, ds_sem)


def copy_bands(*refs):
    half = len(refs) // 2
    for source, target in zip(refs[:half], refs[half:]):
        target[...] = source[...]


def place(n_rep, share, outer_step, parts):
    n_x, n_p = n_rep // 2, len(parts)
    arrays = [part[0] for part in parts]

    def run(step, *refs):
        sources, target, held = refs[:n_p], refs[n_p], refs[n_p + 1:2 * n_p + 1]
        in_sem, out_sem = refs[2 * n_p + 1:]
        rep = lax.axis_index("rep")
        x, core = rep // 2, lax.rem(rep, 2)

        def load(i):
            return pltpu.make_async_copy(sources[i], held[i], in_sem.at[i])

        def store(i):
            array, first, d, other = parts[i]
            owner = 2 * lax.rem(x + d, n_x) + (1 - core if other else core)
            r = pl.ds(pl.multiple_of(owner * share + first, 16), array.shape[0])
            return pltpu.make_async_copy(held[i], target.at[r], out_sem.at[i])

        for i in range(n_p):
            load(i).start()
        for i in range(n_p):
            load(i).wait()
            store(i).start()
        for i in range(n_p):
            store(i).wait()

    moved = sum(array.nbytes for array in arrays)
    return pl.pallas_call(
        run,
        out_shape=jax.ShapeDtypeStruct(outer_step.shape, outer_step.dtype),
        in_specs=[pl.BlockSpec(memory_space=pltpu.HBM)] + [pl.BlockSpec(memory_space=pl.ANY)] * n_p,
        out_specs=pl.BlockSpec(memory_space=pltpu.HBM),
        scratch_shapes=[pltpu.VMEM(array.shape, array.dtype) for array in arrays] + [
            pltpu.SemaphoreType.DMA((n_p,)),
            pltpu.SemaphoreType.DMA((n_p,)),
        ],
        input_output_aliases={0: 0},
        compiler_params=pltpu.CompilerParams(vmem_limit_bytes=whole_vmem),
        cost_estimate=pl.CostEstimate(
            flops=copy_flops * moved, bytes_accessed=2 * moved, transcendentals=0
        ),
        name="place",
    )(outer_step, *arrays)


def per_device(sizes, hidden, down_weight, out_grad, pseudo_grad, momentum):
    n_rep, n_dp, n_tp = sizes
    n_x = n_rep // 2
    tokens = hidden.shape[1]
    ffn, cols = down_weight.shape
    share = momentum.shape[0]
    n_k = pieces(share, 16, 28)
    n_f = pieces(ffn, 128, 14)
    n_late = max(1, (4 * n_k) // 14)
    chunk, fb = share // n_k, ffn // n_f
    late_rows = n_late * chunk
    last = max(16, late_rows // 16 // 16 * 16)
    tail = [4 * last, 2 * last, last]
    if late_rows - sum(tail) < 16:
        tail = [16] * 3
    lengths = [late_rows - sum(tail)] + tail
    groups = tuple((sum(lengths[:g]), lengths[g]) for g in range(n_groups))
    t_rows, d_rows = tokens // n_tp, tokens // n_dp
    dma = pltpu.SemaphoreType.DMA
    out = pl.pallas_call(
        functools.partial(kernel, n_rep, n_dp, n_tp, n_k, n_late, n_f, groups),
        out_shape=(
            jax.ShapeDtypeStruct((1, t_rows, cols), bf16),
            jax.ShapeDtypeStruct((1, d_rows, ffn), bf16),
            jax.ShapeDtypeStruct((share, cols), f32),
            jax.ShapeDtypeStruct((ffn, cols), bf16),
            jax.ShapeDtypeStruct((share, cols), bf16),
        ) + tuple(jax.ShapeDtypeStruct((size, cols), bf16) for _, size in groups)
        + (jax.ShapeDtypeStruct((chunk, cols), bf16),) * (n_x - 1),
        in_specs=[pl.BlockSpec(memory_space=pl.ANY)] * 5,
        out_specs=[pl.BlockSpec(memory_space=pl.ANY)] * (4 + len(groups) + n_x),
        scratch_shapes=[
            pltpu.VMEM((n_x - 1, share, cols), bf16),
            pltpu.VMEM((n_x - 1, share, cols), bf16),
            pltpu.VMEM((n_x - 1, share, cols), bf16),
            pltpu.VMEM((2, chunk, cols), bf16),
            pltpu.VMEM((chunk, cols), bf16),
            pltpu.VMEM((chunk, cols), f32),
            pltpu.VMEM((chunk, cols), f32),
            pltpu.VMEM((fb, cols), bf16),
            pltpu.VMEM((tokens, fb), bf16),
            pltpu.VMEM((tokens, cols), bf16),
            pltpu.VMEM((tokens, cols), f32),
            pltpu.VMEM((tokens, cols), bf16),
            pltpu.VMEM((n_tp - 1, t_rows, cols), bf16),
            pltpu.VMEM((tokens, ffn), bf16),
            pltpu.VMEM((n_dp - 1, d_rows, ffn), bf16),
            dma((4 + len(groups),)),
            dma,
            dma((n_x, n_k)),
            dma,
            dma((n_x - 1, n_k)),
            dma,
            dma((n_x - 1, n_k)),
            dma,
            dma,
            dma,
            dma((n_tp - 1,)),
            dma((n_tp - 1,)),
            dma((n_tp - 1,)),
            dma((n_tp - 1,)),
            dma,
            dma((n_dp - 1,)),
        ],
        compiler_params=pltpu.CompilerParams(
            collective_id=0, has_side_effects=True, vmem_limit_bytes=60 * 2**20
        ),
        name="layer_step",
    )(hidden, down_weight, out_grad, pseudo_grad, momentum)
    layer_out, hidden_grad, new_momentum, outer_step = out[:4]
    late, edge = out[5:5 + len(groups)], out[5 + len(groups):]

    def across(value, d):
        hops = [(2 * x + c, 2 * ((x - d) % n_x) + c) for x in range(n_x) for c in range(2)]
        return lax.ppermute(value, "rep", hops)

    def beside(value):
        hops = [(2 * x + c, 2 * x + 1 - c) for x in range(n_x) for c in range(2)]
        return lax.ppermute(value, "rep", hops)

    arrived = []
    for value in late:
        arrived.append([across(value, d) for d in range(1, n_x)])
    near = [beside(value) for value in late]
    edge_near = [beside(value) for value in edge]
    results = (layer_out, hidden_grad, new_momentum, outer_step)
    steps = max(
        k for k in range(1, 9)
        if not any(n % (16 * k) for n in (t_rows, d_rows, ffn)) and share % (8 * k) == 0
    )

    def band(array):
        block = array.shape[:-2] + (array.shape[-2] // steps, array.shape[-1])
        return pl.BlockSpec(block, lambda i: (0,) * (array.ndim - 2) + (i, 0))

    layer_out, hidden_grad, new_momentum, outer_step = pl.pallas_call(
        copy_bands,
        out_shape=tuple(jax.ShapeDtypeStruct(r.shape, r.dtype) for r in results),
        grid=(steps,),
        in_specs=[band(r) for r in results],
        out_specs=[band(r) for r in results],
        cost_estimate=pl.CostEstimate(
            flops=copy_flops * sum(r.nbytes for r in results),
            bytes_accessed=2 * sum(r.nbytes for r in results), transcendentals=0,
        ),
        compiler_params=pltpu.CompilerParams(vmem_limit_bytes=whole_vmem),
    )(*results)
    firsts = [share - late_rows + start for start, _ in groups]
    parts = []
    for d in range(1, n_x):
        parts.append((edge[d - 1], share - late_rows - chunk, n_x - d, False))
        parts.append((edge_near[d - 1], share - late_rows - chunk, n_x - d, True))
    for first, value, own in zip(firsts, late, near):
        parts += [(value, first, 0, False), (own, first, 0, True)]
    outer_step = place(n_rep, share, outer_step, parts)

    def put(outer_step, values, first, other):
        rep = lax.axis_index("rep")
        x, core = rep // 2, lax.rem(rep, 2)
        for d, value in enumerate(values):
            owner = 2 * lax.rem(x + d + 1, n_x) + (1 - core if other else core)
            outer_step = lax.dynamic_update_slice(outer_step, value, (owner * share + first, 0))
        return outer_step

    for first, here in zip(firsts, arrived):
        here, outer_step = lax.optimization_barrier((here, outer_step))
        across_near = [beside(value) for value in here]
        outer_step = put(outer_step, here, first, False)
        outer_step = put(outer_step, across_near, first, True)
    return layer_out, hidden_grad, new_momentum, outer_step


def solution(mesh):
    sizes = tuple(mesh.shape[a] for a in ("rep", "dp", "tp"))

    def step(*args):
        return per_device(sizes, *args)

    return jax.shard_map(
        step,
        mesh=mesh,
        in_specs=(
            P("rep", None, "tp"),
            P("tp", "dp"),
            P("rep", "tp", "dp"),
            P("rep", "tp", "dp"),
            P(("tp", "rep"), "dp"),
        ),
        out_specs=(
            P("rep", "tp", "dp"),
            P("rep", "dp", "tp"),
            P(("tp", "rep"), "dp"),
            P("tp", "dp"),
        ),
        check_vma=False,
    )
```

```python
import functools

import jax
import jax.numpy as jnp
from jax import lax
from jax.experimental import pallas as pl
from jax.experimental.pallas import tpu as pltpu
from jax.sharding import PartitionSpec as P

outer_rate = 0.7
momentum_rate = 0.9

copy_flops = 1000
n_groups = 4
n_late_of, n_skew_of = 9, 4
whole_vmem = 2**26 - 2**16

MESH = pl.DeviceIdType.MESH
f32 = jnp.float32
bf16 = jnp.bfloat16


def pieces(extent, unit, most):
    return max(k for k in range(1, most + 1) if extent % (k * unit) == 0)


def kernel(
    n_rep, n_dp, n_tp, n_k, n_late, n_skew, n_f, groups,
    hidden, weight, grads, pseudo, momentum,
    layer_out, hidden_grad, new_momentum, outer_step, xch, *refs,
):
    n_x, n_g = n_rep // 2, len(groups)
    late, edge, refs = refs[:n_g], refs[n_g:n_g + n_x - 1], refs[n_g + n_x - 1:]
    body(n_rep, n_dp, n_tp, n_k, n_late, n_skew, n_f, groups,
         hidden, weight, grads, pseudo, momentum,
         layer_out, hidden_grad, new_momentum, outer_step, xch, late, edge, *refs)


def body(
    n_rep, n_dp, n_tp, n_k, n_late, n_skew, n_f, groups,
    hidden, weight, grads, pseudo, momentum,
    layer_out, hidden_grad, new_momentum, outer_step, xch, late, edge,
    ps, pr, xv, la, lb, mom, nmb, wb, hb, gf, acc, po, tr, pb, dr,
    ld_sem, xs_sem, xr_sem, ps_sem, pr_sem, ss_sem, sr_sem, fs_sem, fr_sem, own_sem,
    gs_sem, gr_sem, ts_sem, tr_sem, ds_sem, dr_sem,
):
    n_x = n_rep // 2
    rep, dp, tp = lax.axis_index("rep"), lax.axis_index("dp"), lax.axis_index("tp")
    x, core = rep // 2, lax.rem(rep, 2)
    partner = 2 * x + 1 - core
    share, cols = momentum.shape
    chunk = share // n_k
    ffn = weight.shape[0]
    fb = ffn // n_f
    tokens = hidden.shape[1]
    t_rows, d_rows = tokens // n_tp, tokens // n_dp
    row_unit = 16
    n_sent = n_k - n_late
    n_low = n_sent - n_skew
    sent = pl.ds(0, n_sent * chunk)

    def chip(d):
        return lax.rem(x + d, n_x)

    def rep_peer(d):
        return 2 * chip(d) + core

    def rows(owner, k):
        return pl.ds(pl.multiple_of(owner * share + k * chunk, chunk), chunk)

    def part(k):
        return pl.ds(pl.multiple_of(k * chunk, chunk), chunk)

    def remote(src, dst, send, recv, axis, index):
        return pltpu.make_async_remote_copy(
            src_ref=src, dst_ref=dst, send_sem=send, recv_sem=recv,
            device_id={axis: index}, device_id_type=MESH,
        )

    def drain(ref, sem):
        pltpu.make_async_copy(ref, ref, sem).wait()

    def own_rows(t, slot):
        d, k = 1 + lax.rem(t, n_x - 1), t // (n_x - 1)
        return pltpu.make_async_copy(
            pseudo.at[0, rows(rep_peer(d), k)], la.at[slot], ld_sem.at[slot]
        )

    own_rows(0, 0).start()
    barrier = pltpu.get_barrier_semaphore()
    peers = [("rep", partner)]
    peers += [("rep", rep_peer(d)) for d in range(1, n_x)]
    peers += [("dp", lax.rem(dp + d, n_dp)) for d in range(1, n_dp)]
    peers += [("tp", lax.rem(tp + d, n_tp)) for d in range(1, n_tp)]
    for axis, index in peers:
        pl.semaphore_signal(barrier, inc=1, device_id={axis: index}, device_id_type=MESH)
    pl.semaphore_wait(barrier, len(peers))

    def exchange(d, k):
        return remote(
            pseudo.at[0, rows(2 * chip(d) + 1 - core, k)], xv.at[d - 1, part(k)],
            xs_sem, xr_sem.at[d, k], "rep", partner,
        )

    def own_exchange(k):
        return remote(
            pseudo.at[0, rows(partner, k)], xch.at[part(k)],
            xs_sem, xr_sem.at[0, k], "rep", partner,
        )

    def start_exchange(k, carry):
        for d in range(1, n_x):
            exchange(d, k).start()
        return carry

    def start_own_exchange(k, carry):
        own_exchange(k).start()
        return carry

    lax.fori_loop(0, n_k, start_exchange, 0)

    mine = pl.ds(pl.multiple_of(tp * t_rows, t_rows), t_rows)

    def gather(d):
        return remote(grads.at[0], gf.at[mine], gs_sem.at[d - 1], gr_sem.at[d - 1],
                      "tp", lax.rem(tp + d, n_tp))

    for d in range(1, n_tp):
        gather(d).start()
    own_grads = pltpu.make_async_copy(grads.at[0], gf.at[mine], own_sem)
    own_grads.start()
    lax.fori_loop(0, n_k, start_own_exchange, 0)

    def partial_send(d, k):
        return remote(ps.at[d - 1, part(k)], pr.at[d - 1, part(k)], ps_sem,
                      pr_sem.at[d - 1, k], "rep", rep_peer(d))

    def reduce_chunk(t, carry):
        d, k = 1 + lax.rem(t, n_x - 1), t // (n_x - 1)
        slot = lax.rem(t, 2)

        @pl.when(t + 1 < n_k * (n_x - 1))
        def _():
            own_rows(t + 1, 1 - slot).start()

        own_rows(t, slot).wait()
        exchange(d, k).wait_recv()

        def add(i, c):
            r = pl.ds(pl.multiple_of(i * row_unit, row_unit), row_unit)
            o = pl.ds(pl.multiple_of(k * chunk + i * row_unit, row_unit), row_unit)
            total = la[slot, r, :].astype(f32) + xv[d - 1, o, :].astype(f32)
            ps[d - 1, o, :] = total.astype(bf16)
            return c

        lax.fori_loop(0, chunk // row_unit, add, 0)
        partial_send(d, k).start()
        return carry

    lax.fori_loop(0, n_k * (n_x - 1), reduce_chunk, 0)

    tn = cols // pieces(cols, 128, max(1, cols // 512))
    tm = tokens // pieces(tokens, row_unit, 2)

    def clear(i, carry):
        r = pl.ds(pl.multiple_of(i * row_unit, row_unit), row_unit)
        acc[r, :] = jnp.zeros((row_unit, cols), f32)
        return carry

    lax.fori_loop(0, tokens // row_unit, clear, 0)
    own_grads.wait()
    for d in range(1, n_tp):
        gather(d).wait()

    def back_send(d, f):
        to = lax.rem(dp + d, n_dp)
        c = pl.ds(pl.multiple_of(f * fb, fb), fb)
        return remote(
            pb.at[pl.ds(pl.multiple_of(to * d_rows, d_rows), d_rows), c],
            dr.at[d - 1, :, c], ds_sem, dr_sem.at[d - 1], "dp", to,
        )

    def matmul_block(f, carry):
        c = pl.ds(pl.multiple_of(f * fb, fb), fb)
        a = pltpu.make_async_copy(weight.at[c], wb, ld_sem.at[0])
        b = pltpu.make_async_copy(hidden.at[0, :, c], hb, ld_sem.at[1])
        a.start()
        b.start()
        a.wait()
        b.wait()

        def back(m, z):
            r = pl.ds(pl.multiple_of(m * tm, tm), tm)
            product = lax.dot_general(
                gf[r, :], wb[...], (((1,), (1,)), ((), ())), preferred_element_type=f32
            )
            pb[r, c] = product.astype(bf16)
            return z

        lax.fori_loop(0, tokens // tm, back, 0)
        for d in range(1, n_dp):
            back_send(d, f).start()

        def forward(n, z):
            t = pl.ds(pl.multiple_of(n * tn, tn), tn)
            acc[:, t] += jnp.dot(hb[...], wb[:, t], preferred_element_type=f32)
            return z

        lax.fori_loop(0, cols // tn, forward, 0)
        return carry

    lax.fori_loop(0, n_f, matmul_block, 0)

    def round_out(i, carry):
        r = pl.ds(pl.multiple_of(i * row_unit, row_unit), row_unit)
        po[r, :] = acc[r, :].astype(bf16)
        return carry

    lax.fori_loop(0, tokens // row_unit, round_out, 0)

    def out_send(d):
        to = lax.rem(tp + d, n_tp)
        return remote(po.at[pl.ds(pl.multiple_of(to * t_rows, t_rows), t_rows)],
                      tr.at[d - 1], ts_sem.at[d - 1], tr_sem.at[d - 1], "tp", to)

    for d in range(1, n_tp):
        out_send(d).start()

    def store_momentum(k):
        return pltpu.make_async_copy(nmb, new_momentum.at[part(k)], ld_sem.at[3])

    def step_send(d, k):
        return remote(pr.at[0, part(k)], outer_step.at[rows(rep, k)], ss_sem,
                      sr_sem.at[d - 1, k], "rep", rep_peer(d))

    def edge_send(d, k):
        place_at = pl.ds(pl.multiple_of((k - n_low) * chunk, chunk), chunk)
        return remote(pr.at[0, part(k)], edge[d - 1].at[place_at], ss_sem,
                      sr_sem.at[d - 1, k], "rep", rep_peer(d))

    def update_chunk(k, carry):
        a = pltpu.make_async_copy(pseudo.at[0, rows(rep, k)], la.at[0], ld_sem.at[0])
        m = pltpu.make_async_copy(momentum.at[part(k)], mom, ld_sem.at[2])
        a.start()
        m.start()
        own_exchange(k).wait_recv()
        b = pltpu.make_async_copy(xch.at[part(k)], lb, ld_sem.at[1])
        b.start()
        for d in range(1, n_x):
            partial_send(d, k).wait_recv()

        @pl.when(k > 0)
        def _():
            store_momentum(k - 1).wait()

        a.wait()
        b.wait()
        m.wait()

        def update(i, c):
            r = pl.ds(pl.multiple_of(i * row_unit, row_unit), row_unit)
            o = pl.ds(pl.multiple_of(k * chunk + i * row_unit, row_unit), row_unit)
            total = la[0, r, :].astype(f32) + lb[r, :].astype(f32)
            for d in range(1, n_x):
                total += pr[d - 1, o, :].astype(f32)
            average = total / n_rep
            fresh = momentum_rate * mom[r, :] + average
            nmb[r, :] = fresh
            pr[0, o, :] = (outer_rate * (average + momentum_rate * fresh)).astype(bf16)
            return c

        lax.fori_loop(0, chunk // row_unit, update, 0)

        @pl.when(k < n_low)
        def _():
            for d in range(1, n_x):
                step_send(d, k).start()

        @pl.when((k >= n_low) & (k < n_sent) & (core == 0))
        def _():
            for d in range(1, n_x):
                edge_send(d, k).start()

        @pl.when(k < n_sent)
        def _():
            remote(pr.at[0, part(k)], outer_step.at[rows(rep, k)], fs_sem, fr_sem,
                   "rep", partner).start()
            pltpu.make_async_copy(
                pr.at[0, part(k)], outer_step.at[rows(rep, k)], own_sem
            ).start()

        store_momentum(k).start()
        return carry

    lax.fori_loop(0, n_k, update_chunk, 0)
    store_momentum(n_k - 1).wait()
    late_copies = [
        pltpu.make_async_copy(
            pr.at[0, pl.ds(n_sent * chunk + start, size)], target, ld_sem.at[4 + g]
        )
        for g, ((start, size), target) in enumerate(zip(groups, late))
    ]
    for copy in late_copies:
        copy.start()

    def forward_chunk(k, carry):
        for d in range(1, n_x):
            step_send(d, k).wait_recv()
            r = rows(2 * chip(n_x - d) + core, k)
            remote(outer_step.at[r], outer_step.at[r], fs_sem, fr_sem, "rep", partner).start()
        return carry

    lax.fori_loop(0, n_low // 2, forward_chunk, 0)

    for d in range(1, n_tp):
        out_send(d).wait()

    def sum_out(i, carry):
        r = pl.ds(pl.multiple_of(i * row_unit, row_unit), row_unit)
        o = pl.ds(pl.multiple_of(tp * t_rows + i * row_unit, row_unit), row_unit)
        total = po[o, :].astype(f32)
        for d in range(1, n_tp):
            total += tr[d - 1, r, :].astype(f32)
        tr[0, r, :] = total.astype(bf16)
        return carry

    lax.fori_loop(0, t_rows // row_unit, sum_out, 0)
    out_copy = pltpu.make_async_copy(tr.at[0], layer_out.at[0], ld_sem.at[0])
    out_copy.start()

    for d in range(1, n_dp):
        drain(dr.at[d - 1], dr_sem.at[d - 1])

    def sum_back(f, carry):
        c = pl.ds(pl.multiple_of(f * fb, fb), fb)

        def band(i, z):
            r = pl.ds(pl.multiple_of(i * row_unit, row_unit), row_unit)
            o = pl.ds(pl.multiple_of(dp * d_rows + i * row_unit, row_unit), row_unit)
            total = pb[o, c].astype(f32)
            for d in range(1, n_dp):
                total += dr[d - 1, r, c].astype(f32)
            dr[0, r, c] = total.astype(bf16)
            return z

        lax.fori_loop(0, d_rows // row_unit, band, 0)
        return carry

    lax.fori_loop(0, n_f, sum_back, 0)
    back_copy = pltpu.make_async_copy(dr.at[0], hidden_grad.at[0], ld_sem.at[1])
    back_copy.start()

    lax.fori_loop(n_low // 2, n_low, forward_chunk, 0)

    out_copy.wait()
    back_copy.wait()
    for copy in late_copies:
        copy.wait()
    drain(outer_step.at[pl.ds(0, n_x * share)], xs_sem)
    drain(ps, ps_sem)

    @pl.when(core == 0)
    def _():
        drain(ps.at[:, sent], ss_sem)

    @pl.when(core == 1)
    def _():
        drain(ps.at[:, pl.ds(0, n_low * chunk)], ss_sem)

    forwarded = pl.ds(0, (n_sent + (n_x - 1) * n_low) * chunk)
    drain(outer_step.at[forwarded], fs_sem)
    drain(outer_step.at[forwarded], fr_sem)

    @pl.when(core == 0)
    def _():
        def edge_wait(k, carry):
            for d in range(1, n_x):
                edge_send(d, k).wait_recv()
            return carry

        lax.fori_loop(n_low, n_sent, edge_wait, 0)

    drain(pr.at[0, sent], own_sem)
    drain(dr, ds_sem)


def copy_bands(*refs):
    half = len(refs) // 2
    for source, target in zip(refs[:half], refs[half:]):
        target[...] = source[...]


def place(n_rep, share, outer_step, parts):
    n_x, n_p = n_rep // 2, len(parts)
    arrays = [part[0] for part in parts]

    def run(step, *refs):
        sources, target, held = refs[:n_p], refs[n_p], refs[n_p + 1:2 * n_p + 1]
        in_sem, out_sem = refs[2 * n_p + 1:]
        rep = lax.axis_index("rep")
        x, core = rep // 2, lax.rem(rep, 2)

        def load(i):
            return pltpu.make_async_copy(sources[i], held[i], in_sem.at[i])

        def store(i):
            array, first, d, other = parts[i]
            owner = 2 * lax.rem(x + d, n_x) + (1 - core if other else core)
            r = pl.ds(pl.multiple_of(owner * share + first, 16), array.shape[0])
            return pltpu.make_async_copy(held[i], target.at[r], out_sem.at[i])

        for i in range(n_p):
            load(i).start()
        for i in range(n_p):
            load(i).wait()
            store(i).start()
        for i in range(n_p):
            store(i).wait()

    moved = sum(array.nbytes for array in arrays)
    return pl.pallas_call(
        run,
        out_shape=jax.ShapeDtypeStruct(outer_step.shape, outer_step.dtype),
        in_specs=[pl.BlockSpec(memory_space=pltpu.HBM)] + [pl.BlockSpec(memory_space=pl.ANY)] * n_p,
        out_specs=pl.BlockSpec(memory_space=pltpu.HBM),
        scratch_shapes=[pltpu.VMEM(array.shape, array.dtype) for array in arrays] + [
            pltpu.SemaphoreType.DMA((n_p,)),
            pltpu.SemaphoreType.DMA((n_p,)),
        ],
        input_output_aliases={0: 0},
        compiler_params=pltpu.CompilerParams(vmem_limit_bytes=whole_vmem),
        cost_estimate=pl.CostEstimate(
            flops=copy_flops * moved, bytes_accessed=2 * moved, transcendentals=0
        ),
        name="place",
    )(outer_step, *arrays)


def per_device(sizes, hidden, down_weight, out_grad, pseudo_grad, momentum):
    n_rep, n_dp, n_tp = sizes
    n_x = n_rep // 2
    tokens = hidden.shape[1]
    ffn, cols = down_weight.shape
    share = momentum.shape[0]
    n_k = pieces(share, 16, 28)
    n_f = pieces(ffn, 128, 14)
    n_late = max(1, (n_late_of * n_k) // 28)
    n_skew = max(1, (n_skew_of * n_k) // 28)
    chunk, fb = share // n_k, ffn // n_f
    late_rows = n_late * chunk
    last = max(16, late_rows // 16 // 16 * 16)
    tail = [4 * last, 2 * last, last]
    if late_rows - sum(tail) < 16:
        tail = [16] * 3
    lengths = [late_rows - sum(tail)] + tail
    skew = n_skew * chunk
    groups = ((-skew, skew),) + tuple(
        (sum(lengths[:g]), lengths[g]) for g in range(n_groups)
    )
    t_rows, d_rows = tokens // n_tp, tokens // n_dp
    dma = pltpu.SemaphoreType.DMA
    out = pl.pallas_call(
        functools.partial(kernel, n_rep, n_dp, n_tp, n_k, n_late, n_skew, n_f, groups),
        out_shape=(
            jax.ShapeDtypeStruct((1, t_rows, cols), bf16),
            jax.ShapeDtypeStruct((1, d_rows, ffn), bf16),
            jax.ShapeDtypeStruct((share, cols), f32),
            jax.ShapeDtypeStruct((ffn, cols), bf16),
            jax.ShapeDtypeStruct((share, cols), bf16),
        ) + tuple(jax.ShapeDtypeStruct((size, cols), bf16) for _, size in groups)
        + (jax.ShapeDtypeStruct((skew, cols), bf16),) * (n_x - 1),
        in_specs=[pl.BlockSpec(memory_space=pl.ANY)] * 5,
        out_specs=[pl.BlockSpec(memory_space=pl.ANY)] * (4 + len(groups) + n_x),
        scratch_shapes=[
            pltpu.VMEM((n_x - 1, share, cols), bf16),
            pltpu.VMEM((n_x - 1, share, cols), bf16),
            pltpu.VMEM((n_x - 1, share, cols), bf16),
            pltpu.VMEM((2, chunk, cols), bf16),
            pltpu.VMEM((chunk, cols), bf16),
            pltpu.VMEM((chunk, cols), f32),
            pltpu.VMEM((chunk, cols), f32),
            pltpu.VMEM((fb, cols), bf16),
            pltpu.VMEM((tokens, fb), bf16),
            pltpu.VMEM((tokens, cols), bf16),
            pltpu.VMEM((tokens, cols), f32),
            pltpu.VMEM((tokens, cols), bf16),
            pltpu.VMEM((n_tp - 1, t_rows, cols), bf16),
            pltpu.VMEM((tokens, ffn), bf16),
            pltpu.VMEM((n_dp - 1, d_rows, ffn), bf16),
            dma((4 + len(groups),)),
            dma,
            dma((n_x, n_k)),
            dma,
            dma((n_x - 1, n_k)),
            dma,
            dma((n_x - 1, n_k)),
            dma,
            dma,
            dma,
            dma((n_tp - 1,)),
            dma((n_tp - 1,)),
            dma((n_tp - 1,)),
            dma((n_tp - 1,)),
            dma,
            dma((n_dp - 1,)),
        ],
        compiler_params=pltpu.CompilerParams(
            collective_id=0, has_side_effects=True, vmem_limit_bytes=60 * 2**20
        ),
        name="layer_step",
    )(hidden, down_weight, out_grad, pseudo_grad, momentum)
    layer_out, hidden_grad, new_momentum, outer_step = out[:4]
    late, edge = out[5:5 + len(groups)], out[5 + len(groups):]

    def across(value, d, cores=(0, 1)):
        hops = [(2 * x + c, 2 * ((x - d) % n_x) + c) for x in range(n_x) for c in cores]
        return lax.ppermute(value, "rep", hops)

    def beside(value):
        hops = [(2 * x + c, 2 * x + 1 - c) for x in range(n_x) for c in range(2)]
        return lax.ppermute(value, "rep", hops)

    arrived = []
    for g, value in enumerate(late):
        cores = (1,) if g == 0 else (0, 1)
        arrived.append([across(value, d, cores) for d in range(1, n_x)])
    near = [beside(value) for value in late[1:]]
    results = (layer_out, hidden_grad, new_momentum, outer_step)
    steps = max(
        k for k in range(1, 9)
        if not any(n % (16 * k) for n in (t_rows, d_rows, ffn)) and share % (8 * k) == 0
    )

    def band(array):
        block = array.shape[:-2] + (array.shape[-2] // steps, array.shape[-1])
        return pl.BlockSpec(block, lambda i: (0,) * (array.ndim - 2) + (i, 0))

    layer_out, hidden_grad, new_momentum, outer_step = pl.pallas_call(
        copy_bands,
        out_shape=tuple(jax.ShapeDtypeStruct(r.shape, r.dtype) for r in results),
        grid=(steps,),
        in_specs=[band(r) for r in results],
        out_specs=[band(r) for r in results],
        cost_estimate=pl.CostEstimate(
            flops=copy_flops * sum(r.nbytes for r in results),
            bytes_accessed=2 * sum(r.nbytes for r in results), transcendentals=0,
        ),
        compiler_params=pltpu.CompilerParams(vmem_limit_bytes=whole_vmem),
    )(*results)
    firsts = [share - late_rows + start for start, _ in groups]
    parts = []
    for first, value, own in zip(firsts[1:], late[1:], near):
        parts += [(value, first, 0, False), (own, first, 0, True)]
    outer_step = place(n_rep, share, outer_step, parts)

    def put(outer_step, values, first, other):
        rep = lax.axis_index("rep")
        x, core = rep // 2, lax.rem(rep, 2)
        for d, value in enumerate(values):
            owner = 2 * lax.rem(x + d + 1, n_x) + (1 - core if other else core)
            outer_step = lax.dynamic_update_slice(outer_step, value, (owner * share + first, 0))
        return outer_step

    on_edge = lax.rem(lax.axis_index("rep"), 2) == 0
    for g, (first, here) in enumerate(zip(firsts, arrived)):
        here, outer_step = lax.optimization_barrier((here, outer_step))
        if g == 0:
            here = [jnp.where(on_edge, edge[n_x - 2 - d], value) for d, value in enumerate(here)]
        across_near = [beside(value) for value in here]
        outer_step = put(outer_step, here, first, False)
        outer_step = put(outer_step, across_near, first, True)
    return layer_out, hidden_grad, new_momentum, outer_step


def solution(mesh):
    sizes = tuple(mesh.shape[a] for a in ("rep", "dp", "tp"))

    def step(*args):
        return per_device(sizes, *args)

    return jax.shard_map(
        step,
        mesh=mesh,
        in_specs=(
            P("rep", None, "tp"),
            P("tp", "dp"),
            P("rep", "tp", "dp"),
            P("rep", "tp", "dp"),
            P(("tp", "rep"), "dp"),
        ),
        out_specs=(
            P("rep", "tp", "dp"),
            P("rep", "dp", "tp"),
            P(("tp", "rep"), "dp"),
            P("tp", "dp"),
        ),
        check_vma=False,
    )
```
